32 devices in a mesh: krow: 16 (over z, x, core), kcol: 2 (over y).
Axes of the slice: x: 2, y: 2, z: 4, core: 2. Of those that a mesh axis runs over, the one named last changes fastest.
Arguments:
- green: bfloat16 [4, 2, 16, 4, 256, 256], P(None, None, 'krow', 'kcol'), may hold values from -6 to 6
- screened: float32 [16, 4, 65536], P(None, None, ('krow', 'kcol')), may hold values from 0.1 to 1
Outputs:
- sigma: bfloat16 [4, 2, 16, 4, 256, 256], P(None, None, 'krow', 'kcol')
- dressed: bfloat16 [4, 2, 16, 4, 256, 256], P(None, None, 'krow', 'kcol')
The draws below stay inside these ranges and needn't reach their ends.
All inputs are finite; a program needn't handle non-finite values.
Results may differ from the reference program's by a relative error of at most 0.0053.
Values may be sent and summed in bfloat16 or wider, within the bound.
A program may use at most 64 MiB of HBM per device.

```python
import math
import jax
import jax.numpy as jnp
from jax import lax

NO = 256
NE = 4
K1 = 16
K2 = 4
PAIRS = 65536


def block_levels(own_key, dims, cuts, low, largest):
    def one(position, parts):
        draws = jax.random.uniform(jax.random.fold_in(jax.random.fold_in(own_key, 6), position), (parts,), jnp.float32, low / len(cuts), largest / len(cuts))
        return jnp.repeat(jnp.exp(draws), dims[position] // parts).reshape((-1,) + (1,) * (len(dims) - position - 1))

    factor_of = one(*cuts[0])
    for cut in cuts[1:]:
        factor_of = factor_of * one(*cut)
    return factor_of


def noise(stream_key, shape, scale, reach, pieces=(), kind=jnp.bfloat16):
    level = block_levels(stream_key, shape, pieces, -0.22, 0.18) if pieces else 1.0
    array = jax.random.normal(stream_key, shape, jnp.float32) * scale * level
    return jnp.minimum(jnp.maximum(array, -reach), reach).astype(kind)


def setup_inputs(seed: int = 0) -> dict:
    key_of = jax.random.split(jax.random.key(seed), 3)
    return {
        "green": noise(key_of[0], (NE, 2, K1, K2, NO, NO), 1.0, 6.0, ((2, 16), (3, 2))),
        "screened": jnp.clip(0.1 + 0.9 * jax.random.uniform(key_of[1], (K1, K2, PAIRS), jnp.float32) ** block_levels(key_of[1], (K1, K2, PAIRS), ((2, 32),), -0.2, 0.2), 0.1, 1.0),
    }


full_turn = 2.0 * math.pi


def phase_tables(length, forward):
    step_counter = jnp.arange(length, dtype=jnp.int32)
    product = (step_counter[:, None] * step_counter[None, :]) % length
    angles = full_turn * product.astype(jnp.float32) / length
    if forward:
        return jnp.cos(angles) / length, jnp.sin(angles) / length
    return jnp.cos(angles), -jnp.sin(angles)


def apply_over_axis(matrix, values, along_dim):
    letters = "abcdefgh"[:values.ndim]
    target = letters[:along_dim] + "z" + letters[along_dim + 1:]
    formula = "z" + letters[along_dim] + "," + letters + "->" + target
    return jnp.einsum(formula, matrix, values, precision=lax.Precision.HIGHEST)


def complex_along(state, cosine, sine, along_dim):
    real_part, imag_part = state
    out_real = apply_over_axis(cosine, real_part, along_dim) - apply_over_axis(sine, imag_part, along_dim)
    out_imag = apply_over_axis(sine, real_part, along_dim) + apply_over_axis(cosine, imag_part, along_dim)
    return out_real, out_imag


def matmul_batch(left, right):
    return jnp.einsum('xyij,xyjl->xyil', left, right, precision=lax.Precision.HIGHEST)


def reference(green, screened):
    fwd_one = phase_tables(K1, True)
    fwd_two = phase_tables(K2, True)
    inv_one = phase_tables(K1, False)
    inv_two = phase_tables(K2, False)
    pair_weights = screened.reshape(K1, K2, NO, NO)
    green_rows = jnp.moveaxis(green, 4, 0)
    weight_rows = jnp.moveaxis(pair_weights, 2, 0)

    def one_row(operand_list):
        block, wblock = operand_list
        state = (block[:, 0].astype(jnp.float32), block[:, 1].astype(jnp.float32))
        state = complex_along(state, fwd_one[0], fwd_one[1], 1)
        state = complex_along(state, fwd_two[0], fwd_two[1], 2)
        state = (-wblock * state[0], -wblock * state[1])
        state = complex_along(state, inv_one[0], inv_one[1], 1)
        state = complex_along(state, inv_two[0], inv_two[1], 2)
        return jnp.stack(state, 1).astype(jnp.bfloat16)

    sigma = lax.map(one_row, (green_rows, weight_rows))
    sigma = jnp.moveaxis(sigma, 0, 4)

    def one_energy(operand_list):
        green_value_list, self_energy_values = operand_list
        green_real = green_value_list[0].astype(jnp.float32)
        green_imag = green_value_list[1].astype(jnp.float32)
        self_energy_real = self_energy_values[0].astype(jnp.float32)
        self_energy_imaginary = self_energy_values[1].astype(jnp.float32)
        kern_real = matmul_batch(green_real, self_energy_real) - matmul_batch(green_imag, self_energy_imaginary)
        kern_imag = matmul_batch(green_real, self_energy_imaginary) + matmul_batch(green_imag, self_energy_real)
        kern_real = lax.optimization_barrier(kern_real.astype(jnp.bfloat16)).astype(jnp.float32)
        kern_imag = lax.optimization_barrier(kern_imag.astype(jnp.bfloat16)).astype(jnp.float32)
        corr_real = matmul_batch(kern_real, green_real) - matmul_batch(kern_imag, green_imag)
        corr_imag = matmul_batch(kern_real, green_imag) + matmul_batch(kern_imag, green_real)
        return jnp.stack((green_real + corr_real / NO, green_imag + corr_imag / NO), 0).astype(jnp.bfloat16)

    dressed = lax.map(one_energy, (green, sigma))
    return sigma, dressed
```

```python
import functools
import math

import jax
import jax.numpy as jnp
from jax import lax
from jax.experimental import pallas as pl
from jax.experimental.pallas import tpu as pltpu
from jax.sharding import PartitionSpec as P

SUBLANES = 8
LANES = 128


def turn(values, count, size, sign):
    real, imag = values
    count = count * sign % size
    if count * 8 % size == 0:
        eighth = count * 8 // size
        half = math.sqrt(0.5)
        if eighth == 0:
            return real, imag
        if eighth == 2:
            return -imag, real
        if eighth == 4:
            return -real, -imag
        if eighth == 6:
            return imag, -real
        if eighth == 1:
            return (real - imag) * half, (real + imag) * half
        if eighth == 3:
            return (real + imag) * -half, (real - imag) * half
        if eighth == 5:
            return (imag - real) * half, (real + imag) * -half
        return (real + imag) * half, (imag - real) * half
    angle = 2.0 * math.pi * count / size
    cosine, sine = math.cos(angle), math.sin(angle)
    return real * cosine - imag * sine, real * sine + imag * cosine


def transform(values, sign):
    size = len(values)
    if size == 1:
        return values
    if size % 2:
        out = []
        for target in range(size):
            terms = [turn(v, target * source, size, sign) for source, v in enumerate(values)]
            out.append((sum(t[0] for t in terms), sum(t[1] for t in terms)))
        return out
    even = transform(values[0::2], sign)
    odd = transform(values[1::2], sign)
    low, high = [], []
    for t in range(size // 2):
        real, imag = turn(odd[t], t, size, sign)
        low.append((even[t][0] + real, even[t][1] + imag))
        high.append((even[t][0] - real, even[t][1] - imag))
    return low + high


def kernel(
    grid_dims, mesh_dims, rows,
    green, weights, sigma, dressed,
    arrived, results, middle,
    out_sems, in_sems, back_out_sems, back_in_sems,
):
    one, two = grid_dims
    row_count, column_count = mesh_dims
    devices = row_count * column_count
    energies, _, local, orbitals, _ = green.shape
    local_one, local_two = one // row_count, two // column_count
    my_row, my_column = lax.axis_index("krow"), lax.axis_index("kcol")
    me = my_row * column_count + my_column

    def place(peer):
        return (lax.div(peer, column_count), lax.rem(peer, column_count))

    def strip(owner):
        return pl.ds(pl.multiple_of(owner * rows, rows), rows)

    barrier = pltpu.get_barrier_semaphore()

    @pl.loop(1, devices)
    def _(step):
        pl.semaphore_signal(
            barrier, inc=1, device_id=place(lax.rem(me + step, devices)),
            device_id_type=pl.DeviceIdType.MESH,
        )

    pl.semaphore_wait(barrier, devices - 1)

    @pl.loop(0, energies)
    def _(e):
        @pl.loop(1, devices)
        def _(step):
            peer = lax.rem(me + step, devices)
            pltpu.make_async_remote_copy(
                src_ref=green.at[e, :, :, strip(peer), :],
                dst_ref=arrived.at[e, me],
                send_sem=out_sems.at[e],
                recv_sem=in_sems.at[e],
                device_id=place(peer),
                device_id_type=pl.DeviceIdType.MESH,
            ).start()

    def wait_all(buffer, sem, e):
        part = buffer.at[e, pl.ds(0, devices - 1)]
        pltpu.make_async_copy(part, part, sem.at[e]).wait()

    def slot(k1, k2):
        return (
            (k1 // local_one) * column_count + k2 // local_two,
            (k1 % local_one) * local_two + k2 % local_two,
        )

    scale = -1.0 / (one * two)

    @pl.loop(0, energies)
    def _(e):
        wait_all(arrived, in_sems, e)
        arrived[e, me] = green[e, :, :, strip(me), :]

        @pl.loop(0, orbitals // LANES)
        def _(h):
            lanes = pl.ds(pl.multiple_of(h * LANES, LANES), LANES)
            for k2 in range(two):
                values = []
                for k1 in range(one):
                    s, at = slot(k1, k2)
                    values.append(tuple(
                        arrived[e, s, c, at, :, lanes].astype(jnp.float32) for c in range(2)
                    ))
                for r1, v in enumerate(transform(values, 1)):
                    middle[r1, k2, 0] = v[0]
                    middle[r1, k2, 1] = v[1]
            for r1 in range(one):
                values = transform([(middle[r1, k2, 0], middle[r1, k2, 1]) for k2 in range(two)], 1)
                for r2 in range(two):
                    weight = weights[r1, r2, :, lanes] * scale
                    values[r2] = (values[r2][0] * weight, values[r2][1] * weight)
                for k2, v in enumerate(transform(values, -1)):
                    middle[r1, k2, 0] = v[0]
                    middle[r1, k2, 1] = v[1]
            for k2 in range(two):
                values = [(middle[r1, k2, 0], middle[r1, k2, 1]) for r1 in range(one)]
                for k1, v in enumerate(transform(values, -1)):
                    s, at = slot(k1, k2)
                    for c in range(2):
                        results[e, s, c, at, :, lanes] = v[c].astype(jnp.bfloat16)

        @pl.loop(1, devices)
        def _(step):
            peer = lax.rem(me + step, devices)
            pltpu.make_async_remote_copy(
                src_ref=results.at[e, peer],
                dst_ref=sigma.at[e, :, :, strip(me), :],
                send_sem=back_out_sems.at[e],
                recv_sem=back_in_sems.at[e],
                device_id=place(peer),
                device_id_type=pl.DeviceIdType.MESH,
            ).start()

        sigma[e, :, :, strip(me), :] = results[e, me]

    def times(left, right):
        return jnp.dot(left, right, preferred_element_type=jnp.float32)

    @pl.loop(0, energies)
    def _(e):
        wait_all(results, back_in_sems, e)

        @pl.loop(0, local)
        def _(at):
            g_real, g_imag = green[e, 0, at], green[e, 1, at]
            s_real, s_imag = sigma[e, 0, at], sigma[e, 1, at]
            kern_real = (times(g_real, s_real) - times(g_imag, s_imag)).astype(jnp.bfloat16)
            kern_imag = (times(g_real, s_imag) + times(g_imag, s_real)).astype(jnp.bfloat16)
            corr_real = times(kern_real, g_real) - times(kern_imag, g_imag)
            corr_imag = times(kern_real, g_imag) + times(kern_imag, g_real)
            share = 1.0 / orbitals
            dressed[e, 0, at] = (g_real.astype(jnp.float32) + corr_real * share).astype(jnp.bfloat16)
            dressed[e, 1, at] = (g_imag.astype(jnp.float32) + corr_imag * share).astype(jnp.bfloat16)

    @pl.loop(0, energies)
    def _(e):
        wait_all(arrived, out_sems, e)
        wait_all(results, back_out_sems, e)


def exchange_in_kernel(green, screened):
    mesh_dims = (lax.axis_size("krow"), lax.axis_size("kcol"))
    devices = mesh_dims[0] * mesh_dims[1]
    energies, _, local_one, local_two, orbitals, _ = green.shape
    grid_dims = screened.shape[:2]
    rows = orbitals // devices
    local = local_one * local_two
    flat = (energies, 2, local, orbitals, orbitals)
    weights = screened.reshape(grid_dims + (rows, orbitals))
    block = (energies, devices, 2, local, rows, orbitals)
    vmem = pl.BlockSpec(memory_space=pltpu.VMEM)
    sigma, dressed = pl.pallas_call(
        functools.partial(kernel, grid_dims, mesh_dims, rows),
        out_shape=[jax.ShapeDtypeStruct(flat, jnp.bfloat16)] * 2,
        in_specs=[vmem, vmem],
        out_specs=[vmem, vmem],
        scratch_shapes=[
            pltpu.VMEM(block, jnp.bfloat16),
            pltpu.VMEM(block, jnp.bfloat16),
            pltpu.VMEM(grid_dims + (2, rows, LANES), jnp.float32),
            pltpu.SemaphoreType.DMA((energies,)),
            pltpu.SemaphoreType.DMA((energies,)),
            pltpu.SemaphoreType.DMA((energies,)),
            pltpu.SemaphoreType.DMA((energies,)),
        ],
        compiler_params=pltpu.CompilerParams(collective_id=0, has_side_effects=True),
    )(green.reshape(flat), weights)
    return sigma.reshape(green.shape), dressed.reshape(green.shape)


full_turn = 2.0 * math.pi


def phase_tables(length, forward):
    step_counter = jnp.arange(length, dtype=jnp.int32)
    product = step_counter[:, None] * step_counter[None, :] % length
    angles = full_turn * product.astype(jnp.float32) / length
    if forward:
        return (jnp.cos(angles) / length, jnp.sin(angles) / length)
    return (jnp.cos(angles), -jnp.sin(angles))


def apply_over_axis(matrix, values, along_dim):
    letters = "abcdefgh"[: values.ndim]
    target = letters[:along_dim] + "z" + letters[along_dim + 1 :]
    formula = "z" + letters[along_dim] + "," + letters + "->" + target
    return jnp.einsum(formula, matrix, values, precision=lax.Precision.HIGHEST)


def complex_along(state, cosine, sine, along_dim):
    real_part, imag_part = state
    out_real = apply_over_axis(cosine, real_part, along_dim) - apply_over_axis(
        sine, imag_part, along_dim
    )
    out_imag = apply_over_axis(sine, real_part, along_dim) + apply_over_axis(
        cosine, imag_part, along_dim
    )
    return (out_real, out_imag)


def weigh_back(state, weights, lead_one, lead_two):
    state = (-weights * state[0], -weights * state[1])
    cos_one, sin_one = phase_tables(lead_one, False)
    state = complex_along(state, cos_one, sin_one, 1)
    cos_two, sin_two = phase_tables(lead_two, False)
    state = complex_along(state, cos_two, sin_two, 2)
    return jnp.stack(state, 1).astype(jnp.bfloat16)


def whole_local(pieces, weights):
    state = (pieces[:, 0].astype(jnp.float32), pieces[:, 1].astype(jnp.float32))
    cos_two, sin_two = phase_tables(pieces.shape[3], True)
    state = complex_along(state, cos_two, sin_two, 2)
    cos_one, sin_one = phase_tables(pieces.shape[2], True)
    state = complex_along(state, cos_one, sin_one, 1)
    return weigh_back(state, weights, pieces.shape[2], pieces.shape[3])


def matmul_batch(left, right):
    return jnp.einsum("eklij,ekljm->eklim", left, right, preferred_element_type=jnp.float32)


def per_device(green, screened):
    krow_count = lax.axis_size("krow")
    momentum_column_count = lax.axis_size("kcol")
    orbitals = green.shape[4]
    slice_len = orbitals * green.shape[5] // (krow_count * momentum_column_count)
    blocks = green.reshape(green.shape[:4] + (krow_count, momentum_column_count, slice_len))
    weights = screened.reshape(screened.shape[0], screened.shape[1], 1, 1, screened.shape[2])
    gathered = lax.all_to_all(
        lax.all_to_all(blocks, "krow", split_axis=4, concat_axis=2, tiled=True),
        "kcol",
        split_axis=5,
        concat_axis=3,
        tiled=True,
    )
    middle = whole_local(gathered, weights)
    partway = lax.all_to_all(middle, "krow", split_axis=2, concat_axis=4, tiled=True)
    returned = lax.all_to_all(partway, "kcol", split_axis=3, concat_axis=5, tiled=True)
    sigma = returned.reshape(green.shape)
    green_real = green[:, 0]
    green_imag = green[:, 1]
    self_energy_real = sigma[:, 0]
    self_energy_imaginary = sigma[:, 1]
    kern_real = (
        matmul_batch(green_real, self_energy_real) - matmul_batch(green_imag, self_energy_imaginary)
    ).astype(jnp.bfloat16)
    kern_imag = (
        matmul_batch(green_real, self_energy_imaginary) + matmul_batch(green_imag, self_energy_real)
    ).astype(jnp.bfloat16)
    corr_real = matmul_batch(kern_real, green_real) - matmul_batch(kern_imag, green_imag)
    corr_imag = matmul_batch(kern_real, green_imag) + matmul_batch(kern_imag, green_real)
    dressed_real = green_real.astype(jnp.float32) + corr_real / orbitals
    dressed_imag = green_imag.astype(jnp.float32) + corr_imag / orbitals
    dressed = jnp.stack((dressed_real, dressed_imag), 1).astype(jnp.bfloat16)
    return (sigma, dressed)


def choose(green, screened):
    devices = lax.axis_size("krow") * lax.axis_size("kcol")
    orbitals = green.shape[4]
    if orbitals % (devices * SUBLANES) == 0 and orbitals % LANES == 0:
        return exchange_in_kernel(green, screened)
    return per_device(green, screened)


def solution(mesh):
    placed = (P(None, None, "krow", "kcol", None, None), P(None, None, ("krow", "kcol")))
    return jax.shard_map(
        choose,
        mesh=mesh,
        in_specs=placed,
        out_specs=(
            P(None, None, "krow", "kcol", None, None),
            P(None, None, "krow", "kcol", None, None),
        ),
        check_vma=False,
    )
```

```python
import functools
import math

import jax
import jax.numpy as jnp
from jax import lax
from jax.experimental import pallas as pl
from jax.experimental.pallas import tpu as pltpu
from jax.sharding import PartitionSpec as P

SUBLANES = 8
LANES = 128


def turn(values, count, size, sign):
    real, imag = values
    count = count * sign % size
    if count * 8 % size == 0:
        eighth = count * 8 // size
        half = math.sqrt(0.5)
        if eighth == 0:
            return real, imag
        if eighth == 2:
            return -imag, real
        if eighth == 4:
            return -real, -imag
        if eighth == 6:
            return imag, -real
        if eighth == 1:
            return (real - imag) * half, (real + imag) * half
        if eighth == 3:
            return (real + imag) * -half, (real - imag) * half
        if eighth == 5:
            return (imag - real) * half, (real + imag) * -half
        return (real + imag) * half, (imag - real) * half
    angle = 2.0 * math.pi * count / size
    cosine, sine = math.cos(angle), math.sin(angle)
    return real * cosine - imag * sine, real * sine + imag * cosine


def transform(values, sign):
    size = len(values)
    if size == 1:
        return values
    if size % 2:
        out = []
        for target in range(size):
            terms = [turn(v, target * source, size, sign) for source, v in enumerate(values)]
            out.append((sum(t[0] for t in terms), sum(t[1] for t in terms)))
        return out
    even = transform(values[0::2], sign)
    odd = transform(values[1::2], sign)
    low, high = [], []
    for t in range(size // 2):
        real, imag = turn(odd[t], t, size, sign)
        low.append((even[t][0] + real, even[t][1] + imag))
        high.append((even[t][0] - real, even[t][1] - imag))
    return low + high


def kernel(
    grid_dims, mesh_dims, rows,
    green, weights, sigma, dressed,
    arrived, results, middle, pair_weights,
    out_sems, in_sems, back_out_sems, back_in_sems,
):
    one, two = grid_dims
    row_count, column_count = mesh_dims
    devices = row_count * column_count
    energies, _, local, orbitals, _ = green.shape
    local_one, local_two = one // row_count, two // column_count
    my_row, my_column = lax.axis_index("krow"), lax.axis_index("kcol")
    me = my_row * column_count + my_column

    def place(peer):
        return (lax.div(peer, column_count), lax.rem(peer, column_count))

    def strip(owner):
        return pl.ds(pl.multiple_of(owner * rows, rows), rows)

    barrier = pltpu.get_barrier_semaphore()

    @pl.loop(1, devices)
    def _(step):
        pl.semaphore_signal(
            barrier, inc=1, device_id=place(lax.rem(me + step, devices)),
            device_id_type=pl.DeviceIdType.MESH,
        )

    pl.semaphore_wait(barrier, devices - 1)

    @pl.loop(0, energies)
    def _(e):
        @pl.loop(1, devices)
        def _(step):
            peer = lax.rem(me + step, devices)
            pltpu.make_async_remote_copy(
                src_ref=green.at[e, :, :, strip(peer), :],
                dst_ref=arrived.at[e, me],
                send_sem=out_sems.at[e],
                recv_sem=in_sems.at[e],
                device_id=place(peer),
                device_id_type=pl.DeviceIdType.MESH,
            ).start()

    def wait_all(buffer, sem, e):
        part = buffer.at[e, pl.ds(0, devices - 1)]
        pltpu.make_async_copy(part, part, sem.at[e]).wait()

    def slot(k1, k2):
        return (
            (k1 // local_one) * column_count + k2 // local_two,
            (k1 % local_one) * local_two + k2 % local_two,
        )

    scale = -1.0 / (one * two)

    @pl.loop(0, one)
    def _(r1):
        for r2 in range(two):
            for row in range(rows):
                part = weights[r1, r2:r2 + 1, row * orbitals:(row + 1) * orbitals]
                pair_weights[r1, r2, row:row + 1, :] = part * scale

    @pl.loop(0, energies)
    def _(e):
        wait_all(arrived, in_sems, e)
        arrived[e, me] = green[e, :, :, strip(me), :]

        @pl.loop(0, orbitals // LANES)
        def _(h):
            lanes = pl.ds(pl.multiple_of(h * LANES, LANES), LANES)
            for k2 in range(two):
                values = []
                for k1 in range(one):
                    s, at = slot(k1, k2)
                    values.append(tuple(
                        arrived[e, s, c, at, :, lanes].astype(jnp.float32) for c in range(2)
                    ))
                for r1, v in enumerate(transform(values, 1)):
                    middle[r1, k2, 0] = v[0]
                    middle[r1, k2, 1] = v[1]
            for r1 in range(one):
                values = transform([(middle[r1, k2, 0], middle[r1, k2, 1]) for k2 in range(two)], 1)
                for r2 in range(two):
                    weight = pair_weights[r1, r2, :, lanes]
                    values[r2] = (values[r2][0] * weight, values[r2][1] * weight)
                for k2, v in enumerate(transform(values, -1)):
                    middle[r1, k2, 0] = v[0]
                    middle[r1, k2, 1] = v[1]
            for k2 in range(two):
                values = [(middle[r1, k2, 0], middle[r1, k2, 1]) for r1 in range(one)]
                for k1, v in enumerate(transform(values, -1)):
                    s, at = slot(k1, k2)
                    for c in range(2):
                        results[e, s, c, at, :, lanes] = v[c].astype(jnp.bfloat16)

        @pl.loop(1, devices)
        def _(step):
            peer = lax.rem(me + step, devices)
            pltpu.make_async_remote_copy(
                src_ref=results.at[e, peer],
                dst_ref=sigma.at[e, :, :, strip(me), :],
                send_sem=back_out_sems.at[e],
                recv_sem=back_in_sems.at[e],
                device_id=place(peer),
                device_id_type=pl.DeviceIdType.MESH,
            ).start()

        sigma[e, :, :, strip(me), :] = results[e, me]

    def times(left, right):
        return jnp.dot(left, right, preferred_element_type=jnp.float32)

    @pl.loop(0, energies)
    def _(e):
        wait_all(results, back_in_sems, e)

        @pl.loop(0, local)
        def _(at):
            g_real, g_imag = green[e, 0, at], green[e, 1, at]
            s_real, s_imag = sigma[e, 0, at], sigma[e, 1, at]
            kern_real = (times(g_real, s_real) - times(g_imag, s_imag)).astype(jnp.bfloat16)
            kern_imag = (times(g_real, s_imag) + times(g_imag, s_real)).astype(jnp.bfloat16)
            corr_real = times(kern_real, g_real) - times(kern_imag, g_imag)
            corr_imag = times(kern_real, g_imag) + times(kern_imag, g_real)
            share = 1.0 / orbitals
            dressed[e, 0, at] = (g_real.astype(jnp.float32) + corr_real * share).astype(jnp.bfloat16)
            dressed[e, 1, at] = (g_imag.astype(jnp.float32) + corr_imag * share).astype(jnp.bfloat16)

    @pl.loop(0, energies)
    def _(e):
        wait_all(arrived, out_sems, e)
        wait_all(results, back_out_sems, e)


def exchange_in_kernel(green, screened):
    mesh_dims = (lax.axis_size("krow"), lax.axis_size("kcol"))
    devices = mesh_dims[0] * mesh_dims[1]
    energies, _, local_one, local_two, orbitals, _ = green.shape
    grid_dims = screened.shape[:2]
    rows = orbitals // devices
    local = local_one * local_two
    flat = (energies, 2, local, orbitals, orbitals)
    block = (energies, devices, 2, local, rows, orbitals)
    vmem = pl.BlockSpec(memory_space=pltpu.VMEM)
    sigma, dressed = pl.pallas_call(
        functools.partial(kernel, grid_dims, mesh_dims, rows),
        out_shape=[pltpu.VMEM(flat, jnp.bfloat16)] * 2,
        in_specs=[vmem, vmem],
        out_specs=[vmem, vmem],
        scratch_shapes=[
            pltpu.VMEM(block, jnp.bfloat16),
            pltpu.VMEM(block, jnp.bfloat16),
            pltpu.VMEM(grid_dims + (2, rows, LANES), jnp.float32),
            pltpu.VMEM(grid_dims + (rows, orbitals), jnp.float32),
            pltpu.SemaphoreType.DMA((energies,)),
            pltpu.SemaphoreType.DMA((energies,)),
            pltpu.SemaphoreType.DMA((energies,)),
            pltpu.SemaphoreType.DMA((energies,)),
        ],
        compiler_params=pltpu.CompilerParams(
            collective_id=0, has_side_effects=True, vmem_limit_bytes=12 * math.prod(block)
        ),
    )(green.reshape(flat), screened)
    return sigma.reshape(green.shape), dressed.reshape(green.shape)


full_turn = 2.0 * math.pi


def phase_tables(length, forward):
    step_counter = jnp.arange(length, dtype=jnp.int32)
    product = step_counter[:, None] * step_counter[None, :] % length
    angles = full_turn * product.astype(jnp.float32) / length
    if forward:
        return (jnp.cos(angles) / length, jnp.sin(angles) / length)
    return (jnp.cos(angles), -jnp.sin(angles))


def apply_over_axis(matrix, values, along_dim):
    letters = "abcdefgh"[: values.ndim]
    target = letters[:along_dim] + "z" + letters[along_dim + 1 :]
    formula = "z" + letters[along_dim] + "," + letters + "->" + target
    return jnp.einsum(formula, matrix, values, precision=lax.Precision.HIGHEST)


def complex_along(state, cosine, sine, along_dim):
    real_part, imag_part = state
    out_real = apply_over_axis(cosine, real_part, along_dim) - apply_over_axis(
        sine, imag_part, along_dim
    )
    out_imag = apply_over_axis(sine, real_part, along_dim) + apply_over_axis(
        cosine, imag_part, along_dim
    )
    return (out_real, out_imag)


def weigh_back(state, weights, lead_one, lead_two):
    state = (-weights * state[0], -weights * state[1])
    cos_one, sin_one = phase_tables(lead_one, False)
    state = complex_along(state, cos_one, sin_one, 1)
    cos_two, sin_two = phase_tables(lead_two, False)
    state = complex_along(state, cos_two, sin_two, 2)
    return jnp.stack(state, 1).astype(jnp.bfloat16)


def whole_local(pieces, weights):
    state = (pieces[:, 0].astype(jnp.float32), pieces[:, 1].astype(jnp.float32))
    cos_two, sin_two = phase_tables(pieces.shape[3], True)
    state = complex_along(state, cos_two, sin_two, 2)
    cos_one, sin_one = phase_tables(pieces.shape[2], True)
    state = complex_along(state, cos_one, sin_one, 1)
    return weigh_back(state, weights, pieces.shape[2], pieces.shape[3])


def matmul_batch(left, right):
    return jnp.einsum("eklij,ekljm->eklim", left, right, preferred_element_type=jnp.float32)


def per_device(green, screened):
    krow_count = lax.axis_size("krow")
    momentum_column_count = lax.axis_size("kcol")
    orbitals = green.shape[4]
    slice_len = orbitals * green.shape[5] // (krow_count * momentum_column_count)
    blocks = green.reshape(green.shape[:4] + (krow_count, momentum_column_count, slice_len))
    weights = screened.reshape(screened.shape[0], screened.shape[1], 1, 1, screened.shape[2])
    gathered = lax.all_to_all(
        lax.all_to_all(blocks, "krow", split_axis=4, concat_axis=2, tiled=True),
        "kcol",
        split_axis=5,
        concat_axis=3,
        tiled=True,
    )
    middle = whole_local(gathered, weights)
    partway = lax.all_to_all(middle, "krow", split_axis=2, concat_axis=4, tiled=True)
    returned = lax.all_to_all(partway, "kcol", split_axis=3, concat_axis=5, tiled=True)
    sigma = returned.reshape(green.shape)
    green_real = green[:, 0]
    green_imag = green[:, 1]
    self_energy_real = sigma[:, 0]
    self_energy_imaginary = sigma[:, 1]
    kern_real = (
        matmul_batch(green_real, self_energy_real) - matmul_batch(green_imag, self_energy_imaginary)
    ).astype(jnp.bfloat16)
    kern_imag = (
        matmul_batch(green_real, self_energy_imaginary) + matmul_batch(green_imag, self_energy_real)
    ).astype(jnp.bfloat16)
    corr_real = matmul_batch(kern_real, green_real) - matmul_batch(kern_imag, green_imag)
    corr_imag = matmul_batch(kern_real, green_imag) + matmul_batch(kern_imag, green_real)
    dressed_real = green_real.astype(jnp.float32) + corr_real / orbitals
    dressed_imag = green_imag.astype(jnp.float32) + corr_imag / orbitals
    dressed = jnp.stack((dressed_real, dressed_imag), 1).astype(jnp.bfloat16)
    return (sigma, dressed)


def choose(green, screened):
    devices = lax.axis_size("krow") * lax.axis_size("kcol")
    orbitals = green.shape[4]
    if orbitals % (devices * SUBLANES) == 0 and orbitals % LANES == 0:
        return exchange_in_kernel(green, screened)
    return per_device(green, screened)


def solution(mesh):
    placed = (P(None, None, "krow", "kcol", None, None), P(None, None, ("krow", "kcol")))
    return jax.shard_map(
        choose,
        mesh=mesh,
        in_specs=placed,
        out_specs=(
            P(None, None, "krow", "kcol", None, None),
            P(None, None, "krow", "kcol", None, None),
        ),
        check_vma=False,
    )
```
